32 devices in a mesh: var: 4 (over z), lon: 4 (over x, core), lat: 2 (over y).
Axes of the slice: x: 2, y: 2, z: 4, core: 2. Of those that a mesh axis runs over, the one named last changes fastest.
Arguments:
- fields: bfloat16 [48, 2, 48, 48, 16], P(('var', 'lat'), None, None, 'lon'), may hold values from -6 to 6
- score_table: bfloat16 [48, 16, 8], replicated, may hold values from -120 to 120
- score_bias: float32 [48, 8], replicated, may hold values from -6 to 6
- value_table: bfloat16 [48, 16, 512], replicated, may hold values from -1.5 to 1.5
- value_bias: float32 [48, 512], replicated, may hold values from -6 to 6
- agg_weight: bfloat16 [512, 512], replicated, may hold values from -0.25 to 0.25
- qkv_weight: bfloat16 [2, 512, 1536], replicated, may hold values from -10 to 10
- proj_weight: bfloat16 [2, 512, 512], replicated, may hold values from -0.25 to 0.25
- up_weight: bfloat16 [512, 2048], replicated, may hold values from -0.25 to 0.25
- down_weight: bfloat16 [2048, 512], replicated, may hold values from -0.125 to 0.125
- norm_gains: float32 [4, 512], replicated, may hold values from 0.1 to 1.9
- decode_weight: bfloat16 [512, 768], replicated, may hold values from -0.25 to 0.25
- decode_bias: float32 [768], replicated, may hold values from -3 to 3
Outputs:
- forecast: bfloat16 [2, 48, 48, 768], P(None, ('var', 'lat'), 'lon')
The draws below stay inside these ranges and needn't reach their ends.
All inputs are finite; a program needn't handle non-finite values.
Results may differ from the reference program's by a relative error of at most 0.025.
Values may be sent and summed in bfloat16 or wider, within the bound.
No kernel may reach another device: no remote copies, remote signals or barrier semaphores. Data moves between devices by JAX's collectives and lax.ppermute only.
A program may use at most 128 MiB of HBM per device.

```python
import math
import jax
import jax.numpy as jnp
from jax import lax

D = 512
FF = 2048
HEADS = 8
VARS = 48
PATCH = 16
LEV = 2
WLEV = 2
WLAT = 6
WLON = 12
BLOCKS = 2
LATS = 48
LONS = 48
N_VAR = 4
N_LAT = 2


def draw_score_table(key, part):
    base = jax.random.normal(key, (VARS, PATCH, HEADS), jnp.float32)
    drawn = jnp.clip(base * 0.5, -3.0, 3.0)
    return drawn.astype(jnp.bfloat16)


def draw_qkv_weight(key, part):
    base = jax.random.normal(key, (BLOCKS, D, 3 * D), jnp.float32) / math.sqrt(D)
    drawn = base
    return jnp.clip(drawn, -10.0, 10.0).astype(jnp.bfloat16)


def shard_levels(key, extent, split, least, largest):
    loudness = 1.0
    for dim, shards_of in split:
        draws = jax.random.uniform(jax.random.fold_in(jax.random.fold_in(key, 6), dim), (shards_of,), jnp.float32, least / len(split), largest / len(split))
        loudness = loudness * jnp.repeat(jnp.exp(draws), extent[dim] // shards_of).reshape((-1,) + (1,) * (len(extent) - 1 - dim))
    return loudness


def noise(stream_key, dims, scale, most, cuts=(), kind=jnp.bfloat16):
    level = shard_levels(stream_key, dims, cuts, -0.22, 0.18) if cuts else 1.0
    array = jax.random.normal(stream_key, dims, jnp.float32) * scale * level
    return jnp.minimum(jnp.maximum(array, -most), most).astype(kind)


def setup_inputs(seed: int = 0) -> dict:
    key_list = jax.random.split(jax.random.key(seed), 14)
    fields = noise(key_list[0], (VARS, LEV, LATS, LONS, PATCH), 1.0, 6.0, ((0, 8), (3, 4)))
    score_table = draw_score_table(jax.random.fold_in(key_list[13], 71), 0)
    score_bias = noise(key_list[2], (VARS, HEADS), 1.0, 6.0, (), jnp.float32)
    value_table = noise(key_list[3], (VARS, PATCH, D), PATCH ** -0.5, 1.5)
    value_bias = noise(key_list[4], (VARS, D), 1.0, 6.0, (), jnp.float32)
    agg_weight = noise(key_list[5], (D, D), D ** -0.5, 0.25)
    qkv_weight = draw_qkv_weight(jax.random.fold_in(key_list[13], 71), 0)
    proj_weight = noise(key_list[7], (BLOCKS, D, D), D ** -0.5, 0.25)
    up_weight = noise(key_list[8], (D, FF), D ** -0.5, 0.25)
    down_weight = noise(key_list[9], (FF, D), FF ** -0.5, 0.125)
    norm_gains = jnp.clip(1.0 + 0.18 * jax.random.normal(key_list[10], (4, D), jnp.float32), 0.1, 1.9)
    decode_weight = noise(key_list[11], (D, VARS * PATCH), D ** -0.5, 0.25)
    decode_bias = noise(key_list[12], (VARS * PATCH,), 0.5, 3.0, (), jnp.float32)
    return {"fields": fields, "score_table": score_table, "score_bias": score_bias, "value_table": value_table, "value_bias": value_bias, "agg_weight": agg_weight, "qkv_weight": qkv_weight, "proj_weight": proj_weight, "up_weight": up_weight, "down_weight": down_weight, "norm_gains": norm_gains, "decode_weight": decode_weight, "decode_bias": decode_bias}


EPSILON = 1e-05

def layer_norm(values, norm_gain):
    centre = lax.optimization_barrier(jnp.mean(values, axis=-1, keepdims=True))
    shifted = values - centre
    spread = lax.optimization_barrier(jnp.mean(shifted * shifted, axis=-1, keepdims=True))
    return shifted * lax.rsqrt(spread + EPSILON) * norm_gain

def group_terms(patches, scores, top_score, table, offsets):
    levels, rows, cols, patch_size = patches.shape[1:]
    head_count = scores.shape[-1]
    width = table.shape[-1]

    def add_var(totals, pieces):
        patch, score, tab, offset = pieces
        weights = jnp.exp(score - top_score)
        values = jnp.dot(patch.reshape(-1, patch_size), tab, preferred_element_type=jnp.float32) + offset
        values = values.reshape(levels, rows, cols, head_count, width // head_count)
        return ((totals[0] + weights[..., None] * values, totals[1] + weights), None)
    start = (jnp.zeros((levels, rows, cols, head_count, width // head_count), jnp.float32), jnp.zeros((levels, rows, cols, head_count), jnp.float32))
    sums, _ = lax.scan(add_var, start, (patches, scores, table, offsets))
    return sums

def attend(queries, keys_vals, allowed):
    windows, length, model_width = queries.shape
    head_dim = model_width // HEADS
    query_heads = queries.astype(jnp.float32).reshape(windows, length, HEADS, head_dim)
    key_heads = keys_vals[..., :model_width].astype(jnp.float32).reshape(windows, -1, HEADS, head_dim)
    value_heads = keys_vals[..., model_width:].astype(jnp.float32).reshape(windows, -1, HEADS, head_dim)
    scores = jnp.einsum('bqhd,bkhd->bhqk', query_heads, key_heads) / math.sqrt(head_dim)
    scores = jnp.where(allowed[:, None], scores, -jnp.inf)
    scores = scores - lax.optimization_barrier(jnp.max(scores, axis=-1, keepdims=True))
    raised = jnp.exp(scores)
    weights = (raised / lax.optimization_barrier(jnp.sum(raised, axis=-1, keepdims=True))).astype(jnp.bfloat16)
    context = jnp.einsum('bhqk,bkhd->bqhd', weights.astype(jnp.float32), value_heads)
    return context.astype(jnp.bfloat16).reshape(windows, length, model_width)

def to_windows(source, window_sizes):
    level_size, row_size, col_size = window_sizes
    level_count, row_count, col_count, features = source.shape
    blocked = source.reshape(level_count // level_size, level_size, row_count // row_size, row_size, col_count // col_size, col_size, features)
    blocked = blocked.transpose(0, 2, 4, 1, 3, 5, 6)
    return blocked.reshape(level_count // level_size, -1, level_size * row_size * col_size, features)

def from_windows(windowed, full_shape, window_sizes):
    level_size, row_size, col_size = window_sizes
    level_count, row_count, col_count, features = full_shape
    blocked = windowed.reshape(level_count // level_size, row_count // row_size, col_count // col_size, level_size, row_size, col_size, features)
    return blocked.transpose(0, 3, 1, 4, 2, 5, 6).reshape(full_shape)

def window_block(latent, norm_gain, qkv_part, proj_part, offsets):
    level_shift, row_shift, col_shift = offsets
    sizes = (WLEV, WLAT, WLON)
    normed = layer_norm(latent, norm_gain).astype(jnp.bfloat16)
    projected = jnp.dot(normed, qkv_part, preferred_element_type=jnp.float32).astype(jnp.bfloat16)
    level_ids = (jnp.arange(LEV) + level_shift) // WLEV
    row_ids = (jnp.arange(LATS) + row_shift) // WLAT
    col_ids = (jnp.arange(LONS) + col_shift) % LONS // WLON
    cell_ids = jnp.stack(jnp.broadcast_arrays(level_ids[:, None, None], row_ids[None, :, None], col_ids[None, None, :]), axis=-1)
    rolled = jnp.roll(projected, (-level_shift, -row_shift, -col_shift), axis=(0, 1, 2))
    rolled_ids = jnp.roll(cell_ids, (-level_shift, -row_shift, -col_shift), axis=(0, 1, 2))
    windowed = to_windows(rolled, sizes)
    window_ids = to_windows(rolled_ids, sizes)

    def one_level(pieces):
        block_qkv, block_ids = pieces
        allowed = jnp.all(block_ids[:, :, None, :] == block_ids[:, None, :, :], axis=-1)
        return attend(block_qkv[..., :D], block_qkv[..., D:], allowed)
    context = lax.map(one_level, (windowed, window_ids))
    context = from_windows(context, (LEV, LATS, LONS, D), sizes)
    context = jnp.roll(context, (level_shift, row_shift, col_shift), axis=(0, 1, 2))
    return latent + jnp.dot(context, proj_part, preferred_element_type=jnp.float32)

def reference(fields, score_table, score_bias, value_table, value_bias, agg_weight, qkv_weight, proj_weight, up_weight, down_weight, norm_gains, decode_weight, decode_bias):
    groups = N_VAR * N_LAT
    group_vars = VARS // groups
    head_dim = D // HEADS
    widened = fields.astype(jnp.float32)
    scores = jnp.einsum('vlrcp,vph->vlrch', widened, score_table.astype(jnp.float32)) + score_bias[:, None, None, None, :]
    top_score = lax.optimization_barrier(jnp.max(scores, axis=0))
    grouped_fields = fields.reshape(groups, group_vars, LEV, LATS, LONS, PATCH)
    grouped_scores = scores.reshape(groups, group_vars, LEV, LATS, LONS, HEADS)
    grouped_tables = value_table.reshape(groups, group_vars, PATCH, D)
    grouped_offsets = value_bias.reshape(groups, group_vars, D)

    def add_group(totals, pieces):
        field_part, score_part, table_part, offset_part = pieces
        numerator, denominator = group_terms(field_part, score_part, top_score, table_part, offset_part)
        numerator = lax.optimization_barrier(numerator.astype(jnp.bfloat16)).astype(jnp.float32)
        denominator = lax.optimization_barrier(denominator.astype(jnp.bfloat16)).astype(jnp.float32)
        return ((totals[0] + numerator, totals[1] + denominator), None)
    start = (jnp.zeros((LEV, LATS, LONS, HEADS, head_dim), jnp.float32), jnp.zeros((LEV, LATS, LONS, HEADS), jnp.float32))
    sums, _ = lax.scan(add_group, start, (grouped_fields, grouped_scores, grouped_tables, grouped_offsets))
    pooled = (sums[0] / sums[1][..., None]).reshape(LEV, LATS, LONS, D).astype(jnp.bfloat16)
    latent = jnp.dot(pooled, agg_weight, preferred_element_type=jnp.float32)
    hidden = window_block(latent, norm_gains[0], qkv_weight[0], proj_weight[0], (0, 0, 0))
    mixed = layer_norm(hidden, norm_gains[1]).astype(jnp.bfloat16)
    active = jax.nn.gelu(jnp.dot(mixed, up_weight, preferred_element_type=jnp.float32), approximate=True).astype(jnp.bfloat16)
    latent = hidden + jnp.dot(active, down_weight, preferred_element_type=jnp.float32)
    latent = window_block(latent, norm_gains[2], qkv_weight[1], proj_weight[1], (WLEV // 2, WLAT // 2, WLON // 2))
    final = layer_norm(latent, norm_gains[3]).astype(jnp.bfloat16)
    return (jnp.dot(final, decode_weight, preferred_element_type=jnp.float32) + decode_bias).astype(jnp.bfloat16)
```

```python
import functools

import jax
import jax.numpy as jnp
from jax import lax
from jax.experimental import pallas as pl
from jax.experimental.pallas import tpu as pltpu
from jax.sharding import PartitionSpec as P

WLEV = 2
WLAT = 6
WLON = 12
HALF_ROWS = WLAT // 2
HALF_COLS = WLON // 2
EPSILON = 1e-05
LANES = 128
BIAS_PARTS = 3
MASKED = -1e30
F32 = jnp.float32
BF16 = jnp.bfloat16


def iota(shape, dim):
    return lax.broadcasted_iota(jnp.int32, shape, dim)


def mm(a, b):
    return lax.dot_general(a, b, (((1,), (0,)), ((), ())), preferred_element_type=F32)


def mm_nt(a, b):
    return lax.dot_general(a, b, (((1,), (1,)), ((), ())), preferred_element_type=F32)


def three_parts(values):
    parts = []
    for _ in range(BIAS_PARTS):
        part = values.astype(BF16).astype(F32)
        parts.append(part)
        values = values - part
    return parts


def layer_norm(values, gain):
    centre = jnp.mean(values, axis=-1, keepdims=True)
    shifted = values - centre
    spread = jnp.mean(shifted * shifted, axis=-1, keepdims=True)
    return shifted * lax.rsqrt(spread + EPSILON) * gain


def attend(queries, keys, values, allowed, head_count):
    width = queries.shape[1]
    head_dim = width // head_count
    pairs = []
    low = iota((1, LANES), 1) < head_dim
    scaled = queries * jnp.asarray(head_dim**-0.5, BF16)
    for start in range(0, width, LANES):
        q = scaled[:, start : start + LANES]
        k = keys[:, start : start + LANES]
        v = values[:, start : start + LANES]
        outs = []
        for side in (low, ~low):
            scores = mm_nt(jnp.where(side, q, jnp.zeros_like(q)), k)
            if allowed is not None:
                scores = jnp.where(allowed, scores, MASKED)
            raised = jnp.exp(scores - jnp.max(scores, axis=-1, keepdims=True))
            weights = raised * (1.0 / jnp.sum(raised, axis=-1, keepdims=True))
            outs.append(mm(weights.astype(BF16), v))
        pairs.append(jnp.where(low, outs[0], outs[1]).astype(BF16))
    return jnp.concatenate(pairs, axis=1)


def pack_kernel(fields_ref, out_ref, scratch_ref):
    var_count, levels, cols, patch, rows = fields_ref.shape
    bands = out_ref.shape[0]
    features = var_count * patch
    half_cols = cols // HALF_COLS
    half_rows = rows // bands // HALF_ROWS
    run = HALF_ROWS * HALF_COLS
    block = levels * run
    row_ids = iota((rows * HALF_COLS, rows), 0)
    col_ids = iota((rows * HALF_COLS, rows), 1)
    wanted = (row_ids // run) * HALF_ROWS + (row_ids % run) // HALF_COLS
    picks = [
        ((row_ids % HALF_COLS == step) & (wanted == col_ids)).astype(F32).astype(BF16)
        for step in range(HALF_COLS)
    ]
    scratch_ref[...] = jnp.ones(scratch_ref.shape, F32)
    for level in range(levels):
        for col in range(half_cols):
            total = None
            for step in range(HALF_COLS):
                tile = fields_ref[:, level, col * HALF_COLS + step].reshape(features, rows)
                part = mm_nt(picks[step], tile)
                total = part if total is None else total + part
            for band in range(bands):
                for row in range(half_rows):
                    source = (band * half_rows + row) * run
                    target = (row * half_cols + col) * block + level * run
                    scratch_ref[band, target : target + run, :features] = total[source : source + run]
    for band in range(bands):
        out_ref[band] = scratch_ref[band].astype(BF16)


def feature_var(index, local_vars, patch):
    features = local_vars * patch
    result = jnp.where(index < features, index // patch, 0)
    for part in range(BIAS_PARTS):
        first = features + part * local_vars
        result = jnp.where((index >= first) & (index < first + local_vars), index - first, result)
    return result


def pool(received_ref, table_rows, table_bias, value_ref, value_bias_ref, spread_ref, score_ref, part_ref, head_count):
    bands, cells, lanes = received_ref.shape
    all_vars = value_bias_ref.shape[0]
    width = value_bias_ref.shape[1]
    local_vars = all_vars // bands
    patch = table_rows.shape[0] // head_count
    features = local_vars * patch
    used = features + BIAS_PARTS * local_vars

    bias_rows = jnp.concatenate(three_parts(table_bias), axis=0).astype(BF16)
    stacked = jnp.concatenate([table_rows, bias_rows], axis=0)
    depth = stacked.shape[0]
    row = iota((bands * lanes, all_vars), 0)
    owner = (row // lanes) * local_vars + feature_var(row % lanes, local_vars, patch)
    picks = ((owner == iota((bands * lanes, all_vars), 1)) & (row % lanes < used)).astype(F32).astype(BF16)
    row = iota((bands * lanes, depth), 0) % lanes
    slot = jnp.where(row < features, row % patch, patch + (row - features) // local_vars)
    chosen = (iota((bands * lanes, depth), 1) // head_count) == slot
    table = jnp.where(chosen, mm_nt(picks, stacked), 0.0).astype(BF16)
    width_out = head_count * lanes
    sel = (iota((depth, width_out), 0) % head_count == iota((depth, width_out), 1) // lanes).astype(F32).astype(BF16)
    same = feature_var(iota((lanes, lanes), 0), local_vars, patch) == feature_var(
        iota((lanes, lanes), 1), local_vars, patch
    )
    same = jnp.concatenate([same.astype(F32)] * head_count, axis=1)
    for band in range(bands):
        rows = slice(band * lanes, (band + 1) * lanes)
        spread_ref[rows, :] = (mm(table[rows], sel) * same).astype(BF16)

    for band in range(bands):
        biases = value_bias_ref[band * local_vars : (band + 1) * local_vars, :]
        part_ref[...] = jnp.zeros(part_ref.shape, F32)
        for index, part in enumerate(three_parts(biases)):
            part_ref[index * local_vars : (index + 1) * local_vars, :] = part
        value_ref[band * lanes + features : (band + 1) * lanes, :] = part_ref[...].astype(BF16)

    tops = None
    for band in range(bands):
        scores = mm(received_ref[band], spread_ref[band * lanes : (band + 1) * lanes, :])
        score_ref[band] = scores
        tops = scores if tops is None else jnp.maximum(tops, scores)

    group = 2
    row = iota((group * lanes, lanes), 0) % lanes
    ones = ((row >= features) & (row < features + local_vars)).astype(F32).astype(BF16)
    head_dim = width // head_count
    low = iota((1, lanes), 1) < head_dim
    pooled = []
    for start in range(0, width, lanes):
        outs = []
        for side in range(2):
            head = start // head_dim + side
            columns = slice(head * lanes, (head + 1) * lanes)
            top = jnp.max(tops[:, columns], axis=-1, keepdims=True)
            total = None
            for first in range(0, bands, group):
                terms = [
                    (jnp.exp(score_ref[band, :, columns] - top) * received_ref[band].astype(F32)).astype(BF16)
                    for band in range(first, first + group)
                ]
                right = jnp.concatenate(
                    [value_ref[first * lanes : (first + group) * lanes, start : start + lanes], ones], axis=1
                )
                part = mm(jnp.concatenate(terms, axis=1), right)
                total = part if total is None else total + part
            outs.append(total[:, :lanes] * (1.0 / total[:, lanes:]))
        pooled.append(jnp.where(low, outs[0], outs[1]).astype(BF16))
    return jnp.concatenate(pooled, axis=1)


def first_kernel(
    received_ref, table_ref, table_bias_ref, value_bias_ref, gains_ref,
    value_hbm, agg_hbm, qkv_hbm, proj_hbm, up_hbm, down_hbm,
    normed_ref, latent_ref, l1_ref, l2_ref, s1_ref, s2_ref, c11_ref, c12_ref, c21_ref, c22_ref,
    spread_ref, score_ref, part_ref, value_ref, agg_ref, qkv_ref, proj_ref, up_ref, down_ref, own_ref, sems,
    *, levels, half_rows, half_cols, head_count, lon_axis, band_axes,
):
    bands, cells, lanes = received_ref.shape
    local_features = value_hbm.shape[0] // bands
    copies = [
        pltpu.make_async_copy(
            value_hbm.at[pl.ds(band * local_features, local_features)],
            value_ref.at[pl.ds(band * lanes, local_features)],
            sems.at[5 + band],
        )
        for band in range(bands)
    ]
    pairs = (
        (agg_hbm, agg_ref),
        (qkv_hbm.at[0], qkv_ref),
        (proj_hbm.at[0], proj_ref),
        (up_hbm, up_ref),
        (down_hbm, down_ref),
    )
    weights = [pltpu.make_async_copy(a, b, sems.at[i]) for i, (a, b) in enumerate(pairs)]
    for copy in copies + weights:
        copy.start()
    for copy in copies:
        copy.wait()
    width = agg_hbm.shape[0]
    pooled = pool(
        received_ref, table_ref[...], table_bias_ref[...], value_ref, value_bias_ref, spread_ref, score_ref, part_ref,
        head_count,
    )
    weights[0].wait()
    latent = mm(pooled, agg_ref[...])
    normed = layer_norm(latent, gains_ref[0:1, :]).astype(BF16)
    weights[1].wait()
    qkv = mm(normed, qkv_ref[...]).astype(BF16)
    block = levels * HALF_ROWS * HALF_COLS
    allowed = None
    if half_rows > 2 or half_cols > 2 or levels > WLEV:

        def window(index):
            place = index // block
            level = (index % block) // (HALF_ROWS * HALF_COLS)
            return ((place // half_cols // 2) * half_cols + place % half_cols // 2) * levels + level // WLEV

        allowed = window(iota((cells, cells), 0)) == window(iota((cells, cells), 1))
    context = attend(qkv[:, :width], qkv[:, width : 2 * width], qkv[:, 2 * width :], allowed, head_count)
    weights[2].wait()
    hidden = latent + mm(context, proj_ref[...])
    mixed = layer_norm(hidden, gains_ref[1:2, :]).astype(BF16)
    weights[3].wait()
    active = jax.nn.gelu(mm(mixed, up_ref[...]), approximate=True).astype(BF16)
    weights[4].wait()
    latent = hidden + mm(active, down_ref[...])
    latent_ref[...] = latent
    own = layer_norm(latent, gains_ref[2:3, :])
    normed_ref[...] = own.astype(BF16)
    own_ref[...] = own

    lon_even = lax.axis_index(lon_axis) % 2 == 0
    band_even = lax.axis_index(band_axes) % 2 == 0

    def cut(row, col):
        start = (row * half_cols + col) * block
        return own_ref[start : start + block, :]

    last_row, last_col = half_rows - 1, half_cols - 1
    for row in range(half_rows):
        left, right = cut(row, 0), cut(row, last_col)
        rows = slice(row * block, (row + 1) * block)
        own_ref_rows = (jnp.where(lon_even, right, left), jnp.where(lon_even, left, right))
        score_ref[0, rows, :width] = own_ref_rows[0]
        score_ref[1, rows, :width] = own_ref_rows[1]
    l1_ref[...] = score_ref[0, : half_rows * block, :width].astype(BF16)
    l2_ref[...] = score_ref[1, : half_rows * block, :width].astype(BF16)
    for col in range(half_cols):
        above, below = cut(0, col), cut(last_row, col)
        rows = slice(col * block, (col + 1) * block)
        score_ref[2, rows, :width] = jnp.where(band_even, below, above)
        score_ref[3, rows, :width] = jnp.where(band_even, above, below)
    s1_ref[...] = score_ref[2, : half_cols * block, :width].astype(BF16)
    s2_ref[...] = score_ref[3, : half_cols * block, :width].astype(BF16)
    for s_ref, down_first in (((c11_ref, c12_ref), True), ((c21_ref, c22_ref), False)):
        chosen = band_even if down_first else jnp.logical_not(band_even)
        lefts = jnp.where(chosen, cut(last_row, 0), cut(0, 0))
        rights = jnp.where(chosen, cut(last_row, last_col), cut(0, last_col))
        s_ref[0][...] = jnp.where(lon_even, rights, lefts).astype(BF16)
        s_ref[1][...] = jnp.where(lon_even, lefts, rights).astype(BF16)


def second_kernel(
    normed_ref, latent_ref, l1_ref, l2_ref, s1_ref, s2_ref, c11_ref, c12_ref, c21_ref, c22_ref,
    gains_ref, bias_ref, qkv_hbm, proj_hbm, decode_hbm,
    out_ref, frame_ref, cells_ref, row_ref, qkv_ref, proj_ref, decode_ref, sems,
    *, half_rows, half_cols, head_count, lon_axis, band_axes,
):
    levels = out_ref.shape[0]
    cells, width = normed_ref.shape
    block = levels * HALF_ROWS * HALF_COLS
    run = HALF_ROWS * HALF_COLS
    pairs = ((qkv_hbm.at[1], qkv_ref), (proj_hbm.at[1], proj_ref), (decode_hbm, decode_ref))
    weights = [pltpu.make_async_copy(a, b, sems.at[i]) for i, (a, b) in enumerate(pairs)]
    for copy in weights:
        copy.start()
    lon_even = lax.axis_index(lon_axis) % 2 == 0
    band = lax.axis_index(band_axes)
    band_even = band % 2 == 0
    first_band = band == 0
    last_band = band == lax.axis_size(band_axes) - 1

    right, left = half_cols, -1
    below, above = half_rows, -1
    col1 = jnp.where(lon_even, right, left)
    col2 = jnp.where(lon_even, left, right)
    row1 = jnp.where(band_even, below, above)
    row2 = jnp.where(band_even, above, below)
    chunks = [(normed_ref, [(r, c) for r in range(half_rows) for c in range(half_cols)])]
    chunks += [(l1_ref, [(r, col1) for r in range(half_rows)]), (l2_ref, [(r, col2) for r in range(half_rows)])]
    chunks += [(s1_ref, [(row1, c) for c in range(half_cols)]), (s2_ref, [(row2, c) for c in range(half_cols)])]
    chunks += [(c11_ref, [(row1, col1)]), (c12_ref, [(row1, col2)]), (c21_ref, [(row2, col1)]), (c22_ref, [(row2, col2)])]
    window_cols = half_cols // 2 + 1

    def window_of(row, col):
        return ((row + 1) // 2) * window_cols + (col + 1) // 2

    start = 0
    places = []
    for ref, blocks in chunks:
        size = ref.shape[0]
        frame_ref[start : start + size, :] = ref[...].astype(F32)
        start += size
        places += blocks
    total = start
    key = iota((1, total), 1)
    key_place = key // block
    key_window = jnp.zeros((1, total), jnp.int32)
    for index, (row, col) in enumerate(places):
        window = jnp.asarray(window_of(row, col), jnp.int32)
        if not isinstance(row, int):
            missing = ((row < 0) & first_band) | ((row >= half_rows) & last_band)
            window = jnp.where(missing, -1, window)
        key_window = jnp.where(key_place == index, window, key_window)
    key_id = jnp.where(key_window < 0, -1, key_window * (levels + 1) + ((key % block) // run + WLEV // 2) // WLEV)
    query = iota((cells, 1), 0)
    query_place = query // block
    query_window = window_of(query_place // half_cols, query_place % half_cols)
    query_id = query_window * (levels + 1) + ((query % block) // run + WLEV // 2) // WLEV
    allowed = query_id == key_id

    frame = frame_ref[...].astype(BF16)
    weights[0].wait()
    queries = mm(normed_ref[...], qkv_ref[:, :width]).astype(BF16)
    keys_vals = mm(frame, qkv_ref[:, width:]).astype(BF16)
    context = attend(queries, keys_vals[:, :width], keys_vals[:, width:], allowed, head_count)
    weights[1].wait()
    latent = latent_ref[...] + mm(context, proj_ref[...])
    final = layer_norm(latent, gains_ref[3:4, :]).astype(BF16)
    weights[2].wait()
    cells_ref[...] = mm(final, decode_ref[...]) + bias_ref[...]
    for level in range(levels):
        for row in range(half_rows):
            for step in range(HALF_ROWS):
                for col in range(half_cols):
                    source = (row * half_cols + col) * block + level * run + step * HALF_COLS
                    row_ref[col * HALF_COLS : (col + 1) * HALF_COLS, :] = cells_ref[source : source + HALF_COLS, :]
                out_ref[level, row * HALF_ROWS + step] = row_ref[...].astype(BF16)


def swap_first(index, size):
    return index ^ 1 if (index ^ 1) < size else index


def swap_second(index, size, wrap):
    other = ((index + 1) ^ 1) - 1
    if wrap:
        return other % size
    return other if 0 <= other < size else index


def per_device(
    fields, score_table, score_bias, value_table, value_bias, agg_weight, qkv_weight, proj_weight, up_weight,
    down_weight, norm_gains, decode_weight, decode_bias, *, mesh_shape,
):
    band_axes = ("var", "lat")
    lon_axis = "lon"
    sizes = [mesh_shape[name] for name in ("var", "lon", "lat")]
    bands = sizes[0] * sizes[2]
    local_vars, levels, all_rows, cols, patch = fields.shape
    all_vars, _, head_count = score_table.shape
    width = agg_weight.shape[0]
    hidden_width = up_weight.shape[1]
    out_width = decode_weight.shape[1]
    rows = all_rows // bands
    half_rows, half_cols = rows // HALF_ROWS, cols // HALF_COLS
    cells = levels * rows * cols
    block = levels * HALF_ROWS * HALF_COLS
    features = local_vars * patch
    lanes = LANES
    assert features + BIAS_PARTS * local_vars <= lanes
    vmem = pl.BlockSpec(memory_space=pltpu.VMEM)
    hbm = pl.BlockSpec(memory_space=pltpu.HBM)

    packed = pl.pallas_call(
        pack_kernel,
        out_shape=jax.ShapeDtypeStruct((bands, cells, lanes), BF16),
        in_specs=[vmem],
        out_specs=vmem,
        scratch_shapes=[pltpu.VMEM((bands, cells, lanes), F32)],
        name="pack",
    )(fields.transpose(0, 1, 3, 4, 2))
    received = lax.all_to_all(packed, band_axes, 0, 0, tiled=True)

    side = (half_rows * block, width)
    line = (half_cols * block, width)
    corner = (block, width)
    shapes = [(cells, width), side, side, line, line, corner, corner, corner, corner]
    structs = [jax.ShapeDtypeStruct(s, BF16) for s in shapes]
    structs.insert(1, jax.ShapeDtypeStruct((cells, width), F32))
    normed, latent, *sends = pl.pallas_call(
        functools.partial(
            first_kernel, levels=levels, half_rows=half_rows, half_cols=half_cols, head_count=head_count,
            lon_axis=lon_axis, band_axes=band_axes,
        ),
        out_shape=structs,
        in_specs=[vmem] * 5 + [hbm] * 6,
        out_specs=[vmem] * len(structs),
        scratch_shapes=[
            pltpu.VMEM((bands * lanes, head_count * lanes), BF16),
            pltpu.VMEM((bands, cells, head_count * lanes), F32),
            pltpu.VMEM((lanes - features, width), F32),
            pltpu.VMEM((bands * lanes, width), BF16),
            pltpu.VMEM((width, width), BF16),
            pltpu.VMEM((width, 3 * width), BF16),
            pltpu.VMEM((width, width), BF16),
            pltpu.VMEM((width, hidden_width), BF16),
            pltpu.VMEM((hidden_width, width), BF16),
            pltpu.VMEM((cells, width), F32),
            pltpu.SemaphoreType.DMA((5 + bands,)),
        ],
        name="first",
    )(
        received,
        score_table.transpose(1, 2, 0).reshape(patch * head_count, all_vars),
        score_bias.T,
        value_bias,
        norm_gains,
        value_table.reshape(all_vars * patch, width),
        agg_weight,
        qkv_weight,
        proj_weight,
        up_weight,
        down_weight,
    )

    def swap(array, band_to, lon_to):
        pairs = []
        for var in range(sizes[0]):
            for lon in range(sizes[1]):
                for lat in range(sizes[2]):
                    band = band_to(var * sizes[2] + lat)
                    other = ((band // sizes[2]) * sizes[1] + lon_to(lon)) * sizes[2] + band % sizes[2]
                    pairs.append(((var * sizes[1] + lon) * sizes[2] + lat, other))
        return lax.ppermute(array, ("var", "lon", "lat"), pairs)

    def stay(index):
        return index

    band1 = functools.partial(swap_first, size=bands)
    band2 = functools.partial(swap_second, size=bands, wrap=False)
    lon1 = functools.partial(swap_first, size=sizes[1])
    lon2 = functools.partial(swap_second, size=sizes[1], wrap=True)
    moves = [(stay, lon1), (stay, lon2), (band1, stay), (band2, stay)]
    moves += [(band1, lon1), (band1, lon2), (band2, lon1), (band2, lon2)]
    halos = [swap(array, *move) for array, move in zip(sends, moves, strict=True)]

    total = sum(a.shape[0] for a in halos) + cells
    return pl.pallas_call(
        functools.partial(
            second_kernel, half_rows=half_rows, half_cols=half_cols, head_count=head_count, lon_axis=lon_axis,
            band_axes=band_axes,
        ),
        out_shape=jax.ShapeDtypeStruct((levels, rows, cols, out_width), BF16),
        in_specs=[vmem] * 12 + [hbm] * 3,
        out_specs=vmem,
        scratch_shapes=[
            pltpu.VMEM((total, width), F32),
            pltpu.VMEM((cells, out_width), F32),
            pltpu.VMEM((cols, out_width), F32),
            pltpu.VMEM((width, 3 * width), BF16),
            pltpu.VMEM((width, width), BF16),
            pltpu.VMEM((width, out_width), BF16),
            pltpu.SemaphoreType.DMA((3,)),
        ],
        name="second",
    )(normed, latent, *halos, norm_gains, decode_bias.reshape(1, -1), qkv_weight, proj_weight, decode_weight)


def solution(mesh):
    shape = dict(mesh.shape)
    return jax.shard_map(
        functools.partial(per_device, mesh_shape=shape),
        mesh=mesh,
        in_specs=(P(("var", "lat"), None, None, "lon", None),) + (P(),) * 12,
        out_specs=P(None, ("var", "lat"), "lon", None),
        check_vma=False,
    )
```

```python
import functools

import jax
import jax.numpy as jnp
from jax import lax
from jax.experimental import pallas as pl
from jax.experimental.pallas import tpu as pltpu
from jax.sharding import PartitionSpec as P

WLEV = 2
WLAT = 6
WLON = 12
HALF_ROWS = WLAT // 2
HALF_COLS = WLON // 2
EPSILON = 1e-05
LANES = 128
MIB = 1024 * 1024
BIAS_PARTS = 3
MASKED = -1e30
F32 = jnp.float32
BF16 = jnp.bfloat16


def iota(shape, dim):
    return lax.broadcasted_iota(jnp.int32, shape, dim)


def mm(a, b):
    return lax.dot_general(a, b, (((1,), (0,)), ((), ())), preferred_element_type=F32)


def mm_nt(a, b):
    return lax.dot_general(a, b, (((1,), (1,)), ((), ())), preferred_element_type=F32)


def three_parts(values):
    parts = []
    for _ in range(BIAS_PARTS):
        part = values.astype(BF16).astype(F32)
        parts.append(part)
        values = values - part
    return parts


def layer_norm(values, gain):
    centre = jnp.mean(values, axis=-1, keepdims=True)
    shifted = values - centre
    spread = jnp.mean(shifted * shifted, axis=-1, keepdims=True)
    return shifted * lax.rsqrt(spread + EPSILON) * gain


def stack_heads(queries, low):
    zero = jnp.zeros_like(queries)
    return jnp.concatenate([jnp.where(low, queries, zero), jnp.where(low, zero, queries)], axis=0)


def soft_context(scores, values, low):
    top = functools.reduce(jnp.maximum, [jnp.max(s, axis=-1, keepdims=True) for s in scores])
    raised = [jnp.exp(s - top) for s in scores]
    total = sum(jnp.sum(r, axis=-1, keepdims=True) for r in raised)
    context = sum(mm(r.astype(BF16), v) for r, v in zip(raised, values, strict=True)) * (1.0 / total)
    half = context.shape[0] // 2
    return jnp.where(low, context[:half], context[half:]).astype(BF16)


def attend(queries, keys, values, head_dim):
    low = iota((1, LANES), 1) < head_dim
    scaled = queries * jnp.asarray(head_dim**-0.5, BF16)
    pairs = []
    for start in range(0, queries.shape[1], LANES):
        lanes = slice(start, start + LANES)
        scores = mm_nt(stack_heads(scaled[:, lanes], low), keys[:, lanes])
        pairs.append(soft_context([scores], [values[:, lanes]], low))
    return jnp.concatenate(pairs, axis=1)


def feature_var(index, local_vars, patch):
    features = local_vars * patch
    result = jnp.where(index < features, index // patch, 0)
    for part in range(BIAS_PARTS):
        first = features + part * local_vars
        result = jnp.where((index >= first) & (index < first + local_vars), index - first, result)
    return result


def pack_kernel(
    fields_hbm, table_hbm, table_bias_hbm, value_bias_hbm, value_hbm, out_ref, spread_ref, value_ref,
    fields_ref, table_ref, table_bias_ref, value_bias_ref, part_ref, block_ref, rows_ref, sems,
    *, head_count,
):
    var_count, levels, cols, patch, rows = fields_ref.shape
    bands = out_ref.shape[0]
    features = var_count * patch
    smalls = ((table_hbm, table_ref), (table_bias_hbm, table_bias_ref), (value_bias_hbm, value_bias_ref))
    copies = [pltpu.make_async_copy(a, b, sems.at[i]) for i, (a, b) in enumerate(smalls)]
    copies.append(pltpu.make_async_copy(fields_hbm, fields_ref, sems.at[3]))
    for band in range(bands):
        source = value_hbm.at[pl.ds(band * features, features)]
        copies.append(pltpu.make_async_copy(source, value_ref.at[pl.ds(band * LANES, features)], sems.at[4 + band]))
    for copy in copies:
        copy.start()
    copies[0].wait()
    copies[1].wait()
    spread_tables(table_ref[...], table_bias_ref[...], spread_ref, bands, patch, head_count)
    copies[2].wait()
    for band in range(bands):
        biases = value_bias_ref[band * var_count : (band + 1) * var_count, :]
        part_ref[...] = jnp.zeros(part_ref.shape, F32)
        for index, part in enumerate(three_parts(biases)):
            part_ref[index * var_count : (index + 1) * var_count, :] = part
        value_ref[band * LANES + features : (band + 1) * LANES, :] = part_ref[...].astype(BF16)

    run = HALF_ROWS * HALF_COLS
    block = levels * run
    row_ids = iota((rows * HALF_COLS, rows), 0)
    col_ids = iota((rows * HALF_COLS, rows), 1)
    wanted = (row_ids // run) * HALF_ROWS + (row_ids % run) // HALF_COLS
    picks = [
        ((row_ids % HALF_COLS == step) & (wanted == col_ids)).astype(F32).astype(BF16)
        for step in range(HALF_COLS)
    ]
    copies[3].wait()
    for level in range(levels):
        for col in range(2):
            total = None
            for step in range(HALF_COLS):
                tile = fields_ref[:, level, col * HALF_COLS + step].reshape(features, rows)
                part = mm_nt(picks[step], tile)
                total = part if total is None else total + part
            for band in range(bands):
                for row in range(2):
                    source = (band * 2 + row) * run
                    target = (row * 2 + col) * block + level * run
                    block_ref[band, target : target + run, :features] = total[source : source + run]
    lane = iota((1, LANES), 1)
    row_sets = rows_ref.shape[0] // block
    for band in range(bands):
        pieces = [[] for _ in range(row_sets + 1)]
        for place in range(4):
            first, offset = divmod(place * features, LANES)
            data = block_ref[band, place * block : (place + 1) * block, :]
            data = pltpu.roll(data, offset, axis=1) if offset else data
            pieces[first].append((offset, data))
            if offset + features > LANES:
                pieces[first + 1].append((0, data))
        for index in range(row_sets):
            merged = None
            for offset, data in pieces[index]:
                merged = data if merged is None else jnp.where(lane >= offset, data, merged)
            rows_ref[index * block : (index + 1) * block, :] = merged
        out_ref[band] = rows_ref[...].astype(BF16)
    for copy in copies[4:]:
        copy.wait()


def spread_tables(table_rows, table_bias, spread_ref, bands, patch, head_count):
    all_vars = table_bias.shape[1]
    local_vars = all_vars // bands
    features = local_vars * patch
    used = features + BIAS_PARTS * local_vars
    bias_rows = jnp.concatenate(three_parts(table_bias), axis=0).astype(BF16)
    stacked = jnp.concatenate([table_rows, bias_rows], axis=0)
    depth = stacked.shape[0]
    row = iota((bands * LANES, all_vars), 0)
    owner = (row // LANES) * local_vars + feature_var(row % LANES, local_vars, patch)
    picks = ((owner == iota((bands * LANES, all_vars), 1)) & (row % LANES < used)).astype(F32).astype(BF16)
    row = iota((bands * LANES, depth), 0) % LANES
    slot = jnp.where(row < features, row % patch, patch + (row - features) // local_vars)
    chosen = (iota((bands * LANES, depth), 1) // head_count) == slot
    table = jnp.where(chosen, mm_nt(picks, stacked), 0.0).astype(BF16)
    width = head_count * LANES
    select = (iota((depth, width), 0) % head_count == iota((depth, width), 1) // LANES).astype(F32).astype(BF16)
    same = feature_var(iota((LANES, LANES), 0), local_vars, patch) == feature_var(
        iota((LANES, LANES), 1), local_vars, patch
    )
    same = jnp.concatenate([same.astype(F32)] * head_count, axis=1)
    for band in range(bands):
        rows = slice(band * LANES, (band + 1) * LANES)
        spread_ref[rows, :] = (mm(table[rows], select) * same).astype(BF16)


def unpack(received_ref, rows_ref, cells_ref, block, features):
    lane = iota((1, LANES), 1)
    for band in range(received_ref.shape[0]):
        rows_ref[...] = received_ref[band].astype(F32)
        for place in range(4):
            first, offset = divmod(place * features, LANES)
            data = rows_ref[first * block : (first + 1) * block, :]
            if offset + features > LANES:
                data = jnp.where(lane >= offset, data, rows_ref[(first + 1) * block : (first + 2) * block, :])
            data = pltpu.roll(data, LANES - offset, axis=1) if offset else data
            cells_ref[band, place * block : (place + 1) * block, :] = jnp.where(lane < features, data, 1.0)


def pool(cells_ref, spread_ref, value_ref, score_ref, local_vars, features, head_count):
    bands = cells_ref.shape[0]
    width = value_ref.shape[1]
    tops = None
    for band in range(bands):
        scores = mm(cells_ref[band].astype(BF16), spread_ref[band * LANES : (band + 1) * LANES, :])
        score_ref[band] = scores
        tops = scores if tops is None else jnp.maximum(tops, scores)

    group = 2
    row = iota((group * LANES, LANES), 0) % LANES
    ones = ((row >= features) & (row < features + local_vars)).astype(F32).astype(BF16)
    head_dim = width // head_count
    low = iota((1, LANES), 1) < head_dim
    pooled = []
    for start in range(0, width, LANES):
        outs = []
        for side in range(2):
            head = start // head_dim + side
            columns = slice(head * LANES, (head + 1) * LANES)
            top = jnp.max(tops[:, columns], axis=-1, keepdims=True)
            total = None
            for first in range(0, bands, group):
                terms = [
                    (jnp.exp(score_ref[band, :, columns] - top) * cells_ref[band]).astype(BF16)
                    for band in range(first, first + group)
                ]
                right = jnp.concatenate(
                    [value_ref[first * LANES : (first + group) * LANES, start : start + LANES], ones], axis=1
                )
                part = mm(jnp.concatenate(terms, axis=1), right)
                total = part if total is None else total + part
            outs.append(total[:, :LANES] * (1.0 / total[:, LANES:]))
        pooled.append(jnp.where(low, outs[0], outs[1]).astype(BF16))
    return jnp.concatenate(pooled, axis=1)


def first_kernel(
    received_ref, spread_ref, value_ref, gains_hbm, agg_hbm, qkv_hbm, proj_hbm, up_hbm, down_hbm,
    normed_ref, latent_ref, l1_ref, l2_ref, s1_ref, s2_ref, c11_ref, c12_ref, c21_ref, c22_ref,
    rows_ref, cells_ref, score_ref, gains_ref, agg_ref, qkv_ref, proj_ref, up_ref, down_ref, own_ref, sems,
    *, local_vars, features, head_count, lon_axis, band_axes,
):
    pairs = (
        (agg_hbm, agg_ref),
        (gains_hbm, gains_ref),
        (qkv_hbm.at[0], qkv_ref),
        (proj_hbm.at[0], proj_ref),
        (up_hbm, up_ref),
        (down_hbm, down_ref),
    )
    weights = [pltpu.make_async_copy(a, b, sems.at[i]) for i, (a, b) in enumerate(pairs)]
    for copy in weights:
        copy.start()
    width = agg_hbm.shape[0]
    block = cells_ref.shape[1] // 4
    unpack(received_ref, rows_ref, cells_ref, block, features)
    pooled = pool(cells_ref, spread_ref, value_ref, score_ref, local_vars, features, head_count)
    weights[0].wait()
    latent = mm(pooled, agg_ref[...])
    weights[1].wait()
    normed = layer_norm(latent, gains_ref[0:1, :]).astype(BF16)
    weights[2].wait()
    qkv = mm(normed, qkv_ref[...]).astype(BF16)
    context = attend(qkv[:, :width], qkv[:, width : 2 * width], qkv[:, 2 * width :], width // head_count)
    weights[3].wait()
    hidden = latent + mm(context, proj_ref[...])
    mixed = layer_norm(hidden, gains_ref[1:2, :]).astype(BF16)
    weights[4].wait()
    active = jax.nn.gelu(mm(mixed, up_ref[...]), approximate=True).astype(BF16)
    weights[5].wait()
    latent = hidden + mm(active, down_ref[...])
    latent_ref[...] = latent
    own = layer_norm(latent, gains_ref[2:3, :])
    normed_ref[...] = own.astype(BF16)
    own_ref[...] = own

    lon_even = lax.axis_index(lon_axis) % 2 == 0
    band_even = lax.axis_index(band_axes) % 2 == 0
    b00, b01, b10, b11 = (own_ref[i * block : (i + 1) * block, :] for i in range(4))
    side0, other0 = jnp.where(lon_even, b01, b00), jnp.where(lon_even, b00, b01)
    side1, other1 = jnp.where(lon_even, b11, b10), jnp.where(lon_even, b10, b11)
    for ref, (top, bottom) in ((l1_ref, (side0, side1)), (l2_ref, (other0, other1))):
        own_ref[:block, :] = top
        own_ref[block : 2 * block, :] = bottom
        ref[...] = own_ref[: 2 * block, :].astype(BF16)
    half = cells_ref.shape[1] // 2
    upper, lower = normed_ref[:half, :], normed_ref[half:, :]
    s1_ref[...] = jnp.where(band_even, lower, upper)
    s2_ref[...] = jnp.where(band_even, upper, lower)
    c11_ref[...] = jnp.where(band_even, side1, side0).astype(BF16)
    c12_ref[...] = jnp.where(band_even, other1, other0).astype(BF16)
    c21_ref[...] = jnp.where(band_even, side0, side1).astype(BF16)
    c22_ref[...] = jnp.where(band_even, other0, other1).astype(BF16)


def own_kernel(normed_ref, qkv_ref, query_ref, key_ref, value_ref, stack_ref, *, head_count):
    cells, width = normed_ref.shape
    half = cells // 2
    head_dim = width // head_count
    low = iota((1, LANES), 1) < head_dim
    qkv = mm(normed_ref[...], qkv_ref[1])
    queries = qkv[:, :width].astype(BF16).astype(F32) * head_dim**-0.5
    for group in range(2):
        rows = slice(group * half, (group + 1) * half)
        key_ref[group] = qkv[rows, width : 2 * width].astype(BF16)
        value_ref[group] = qkv[rows, 2 * width :].astype(BF16)
        for pair in range(width // LANES):
            stack_ref[...] = stack_heads(queries[rows, pair * LANES : (pair + 1) * LANES], low)
            query_ref[group, pair] = stack_ref[...].astype(BF16)


def second_kernel(
    query_ref, key_ref, value_ref, latent_ref, l1_ref, l2_ref, s1_ref, s2_ref, c11_ref, c12_ref, c21_ref, c22_ref,
    gains_ref, bias_ref, qkv_ref, proj_ref, decode_ref, out_ref, frame_ref, cells_ref,
    *, head_count, lon_axis, band_axes,
):
    levels = out_ref.shape[2]
    cells, width = latent_ref.shape
    half = cells // 2
    head_dim = width // head_count
    run = HALF_ROWS * HALF_COLS
    block = levels * run
    halo = 6 * block
    lon_even = lax.axis_index(lon_axis) % 2 == 0
    band = lax.axis_index(band_axes)
    band_even = band % 2 == 0
    edges = (band == 0, band == lax.axis_size(band_axes) - 1)

    for group in range(2):
        start = group * halo
        swapped = band_even if group == 0 else jnp.logical_not(band_even)
        frame_ref[start : start + block, :] = l1_ref[group * block : (group + 1) * block, :].astype(F32)
        frame_ref[start + block : start + 2 * block, :] = l2_ref[group * block : (group + 1) * block, :].astype(F32)
        line = jnp.where(swapped, s2_ref[...], s1_ref[...])
        frame_ref[start + 2 * block : start + 4 * block, :] = line.astype(F32)
        frame_ref[start + 4 * block : start + 5 * block, :] = jnp.where(swapped, c21_ref[...], c11_ref[...]).astype(F32)
        frame_ref[start + 5 * block : start + 6 * block, :] = jnp.where(swapped, c22_ref[...], c12_ref[...]).astype(F32)
    keys_vals = mm(frame_ref[...].astype(BF16), qkv_ref[1, :, width:])

    def level_of(index):
        return ((index % block) // run + WLEV // 2) // WLEV

    first = jnp.where(lon_even, 1, 0)
    query = iota((2 * half, 1), 0) % half
    own_key = iota((1, half), 1)
    own_allowed = (query // block * levels + level_of(query)) == (own_key // block * levels + level_of(own_key))
    key = iota((1, halo), 1)
    place = key // block
    side = jnp.where((place == 0) | (place == 4), first, jnp.where((place == 1) | (place == 5), 1 - first, place - 2))
    low = iota((1, LANES), 1) < head_dim
    groups = []
    for group in range(2):
        missing = (place >= 2) & edges[group]
        key_id = jnp.where(missing, -1, side * levels + level_of(key))
        allowed = (query // block * levels + level_of(query)) == key_id
        halo_keys = keys_vals[group * halo : (group + 1) * halo, :width].astype(BF16)
        halo_values = keys_vals[group * halo : (group + 1) * halo, width:].astype(BF16)
        pairs = []
        for pair in range(width // LANES):
            lanes = slice(pair * LANES, (pair + 1) * LANES)
            queries = query_ref[group, pair]
            scores = [
                jnp.where(own_allowed, mm_nt(queries, key_ref[group, :, lanes]), MASKED),
                jnp.where(allowed, mm_nt(queries, halo_keys[:, lanes]), MASKED),
            ]
            pairs.append(soft_context(scores, [value_ref[group, :, lanes], halo_values[:, lanes]], low))
        groups.append(mm(jnp.concatenate(pairs, axis=1), proj_ref[1]))
    latent = latent_ref[...] + jnp.concatenate(groups, axis=0)
    final = layer_norm(latent, gains_ref[3:4, :]).astype(BF16)
    decoded = mm(final, decode_ref[...]) + bias_ref[...].reshape(1, -1)
    for index in range(cells_ref.shape[0]):
        cells_ref[index] = decoded[:, index * LANES : (index + 1) * LANES]
    for place in range(4):
        for cell in range(run):
            source = place * block + cell
            out_row = (place // 2) * HALF_ROWS + cell // HALF_COLS
            out_col = (place % 2) * HALF_COLS + cell % HALF_COLS
            for index in range(cells_ref.shape[0]):
                piece = cells_ref[index, pl.ds(source, levels, stride=run), :].astype(BF16)
                out_ref[out_row, out_col, :, index * LANES : (index + 1) * LANES] = piece


def swap_first(index, size):
    return index ^ 1 if (index ^ 1) < size else index


def swap_second(index, size, wrap):
    other = ((index + 1) ^ 1) - 1
    if wrap:
        return other % size
    return other if 0 <= other < size else index


def per_device(
    fields, score_table, score_bias, value_table, value_bias, agg_weight, qkv_weight, proj_weight, up_weight,
    down_weight, norm_gains, decode_weight, decode_bias, *, mesh_shape,
):
    band_axes = ("var", "lat")
    lon_axis = "lon"
    sizes = [mesh_shape[name] for name in ("var", "lon", "lat")]
    bands = sizes[0] * sizes[2]
    local_vars, levels, all_rows, cols, patch = fields.shape
    all_vars, _, head_count = score_table.shape
    width = agg_weight.shape[0]
    hidden_width = up_weight.shape[1]
    out_width = decode_weight.shape[1]
    rows = all_rows // bands
    cells = levels * rows * cols
    block = levels * HALF_ROWS * HALF_COLS
    features = local_vars * patch
    assert rows == WLAT and cols == WLON and levels % WLEV == 0 and features + BIAS_PARTS * local_vars <= LANES
    packed_rows = -(-4 * features // LANES) * block
    vmem = pl.BlockSpec(memory_space=pltpu.VMEM)
    hbm = pl.BlockSpec(memory_space=pltpu.HBM)

    def in_hbm(*arrays):
        return [pltpu.with_memory_space_constraint(array, pltpu.HBM) for array in arrays]

    packed, spread, values = pl.pallas_call(
        functools.partial(pack_kernel, head_count=head_count),
        out_shape=[
            jax.ShapeDtypeStruct((bands, packed_rows, LANES), BF16),
            jax.ShapeDtypeStruct((bands * LANES, head_count * LANES), BF16),
            jax.ShapeDtypeStruct((bands * LANES, width), BF16),
        ],
        in_specs=[hbm] * 5,
        out_specs=[vmem] * 3,
        scratch_shapes=[
            pltpu.VMEM((local_vars, levels, cols, patch, all_rows), BF16),
            pltpu.VMEM((patch * head_count, all_vars), BF16),
            pltpu.VMEM((head_count, all_vars), F32),
            pltpu.VMEM((all_vars, width), F32),
            pltpu.VMEM((LANES - features, width), F32),
            pltpu.VMEM((bands, cells, LANES), F32),
            pltpu.VMEM((packed_rows, LANES), F32),
            pltpu.SemaphoreType.DMA((4 + bands,)),
        ],
        compiler_params=pltpu.CompilerParams(vmem_limit_bytes=16 * MIB),
        name="pack",
    )(
        *in_hbm(
            fields.transpose(0, 1, 3, 4, 2),
            score_table.transpose(1, 2, 0).reshape(patch * head_count, all_vars),
            score_bias.T,
            value_bias,
            value_table.reshape(all_vars * patch, width),
        )
    )
    received = lax.all_to_all(packed, band_axes, 0, 0, tiled=True)

    pair = (2 * block, width)
    corner = (block, width)
    structs = [jax.ShapeDtypeStruct((cells, width), BF16), jax.ShapeDtypeStruct((cells, width), F32)]
    structs += [jax.ShapeDtypeStruct(s, BF16) for s in (pair, pair, pair, pair, corner, corner, corner, corner)]
    normed, latent, *sends = pl.pallas_call(
        functools.partial(
            first_kernel, local_vars=local_vars, features=features, head_count=head_count, lon_axis=lon_axis,
            band_axes=band_axes,
        ),
        out_shape=structs,
        in_specs=[vmem] * 3 + [hbm] * 6,
        out_specs=[vmem] * len(structs),
        scratch_shapes=[
            pltpu.VMEM((packed_rows, LANES), F32),
            pltpu.VMEM((bands, cells, LANES), F32),
            pltpu.VMEM((bands, cells, head_count * LANES), F32),
            pltpu.VMEM(norm_gains.shape, F32),
            pltpu.VMEM((width, width), BF16),
            pltpu.VMEM((width, 3 * width), BF16),
            pltpu.VMEM((width, width), BF16),
            pltpu.VMEM((width, hidden_width), BF16),
            pltpu.VMEM((hidden_width, width), BF16),
            pltpu.VMEM((cells, width), F32),
            pltpu.SemaphoreType.DMA((6,)),
        ],
        compiler_params=pltpu.CompilerParams(vmem_limit_bytes=26 * MIB),
        name="first",
    )(
        received, spread, values,
        *in_hbm(norm_gains, agg_weight, qkv_weight, proj_weight, up_weight, down_weight),
    )

    def swap(array, band_to, lon_to):
        pairs = []
        for var in range(sizes[0]):
            for lon in range(sizes[1]):
                for lat in range(sizes[2]):
                    band = band_to(var * sizes[2] + lat)
                    other = ((band // sizes[2]) * sizes[1] + lon_to(lon)) * sizes[2] + band % sizes[2]
                    pairs.append(((var * sizes[1] + lon) * sizes[2] + lat, other))
        return lax.ppermute(array, ("var", "lon", "lat"), pairs)

    def stay(index):
        return index

    band1 = functools.partial(swap_first, size=bands)
    band2 = functools.partial(swap_second, size=bands, wrap=False)
    lon1 = functools.partial(swap_first, size=sizes[1])
    lon2 = functools.partial(swap_second, size=sizes[1], wrap=True)
    moves = [(stay, lon1), (stay, lon2), (band1, stay), (band2, stay)]
    moves += [(band1, lon1), (band1, lon2), (band2, lon1), (band2, lon2)]
    halos = [swap(array, *move) for array, move in zip(sends, moves, strict=True)]

    half = cells // 2
    queries, keys, vals = pl.pallas_call(
        functools.partial(own_kernel, head_count=head_count),
        out_shape=[
            jax.ShapeDtypeStruct((2, width // LANES, cells, LANES), BF16),
            jax.ShapeDtypeStruct((2, half, width), BF16),
            jax.ShapeDtypeStruct((2, half, width), BF16),
        ],
        in_specs=[vmem] * 2,
        out_specs=[vmem] * 3,
        scratch_shapes=[pltpu.VMEM((cells, LANES), F32)],
        compiler_params=pltpu.CompilerParams(vmem_limit_bytes=12 * MIB),
        name="own",
    )(normed, qkv_weight)
    forecast = pl.pallas_call(
        functools.partial(second_kernel, head_count=head_count, lon_axis=lon_axis, band_axes=band_axes),
        out_shape=jax.ShapeDtypeStruct((rows, cols, levels, out_width), BF16),
        in_specs=[vmem] * 17,
        out_specs=vmem,
        scratch_shapes=[pltpu.VMEM((12 * block, width), F32), pltpu.VMEM((out_width // LANES, cells, LANES), F32)],
        compiler_params=pltpu.CompilerParams(vmem_limit_bytes=20 * MIB),
        name="second",
    )(queries, keys, vals, latent, *halos, norm_gains, decode_bias, qkv_weight, proj_weight, decode_weight)
    return forecast.transpose(2, 0, 1, 3)


def solution(mesh):
    shape = dict(mesh.shape)
    return jax.shard_map(
        functools.partial(per_device, mesh_shape=shape),
        mesh=mesh,
        in_specs=(P(("var", "lat"), None, None, "lon", None),) + (P(),) * 12,
        out_specs=P(None, ("var", "lat"), "lon", None),
        check_vma=False,
    )
```

```python
import functools

import jax
import jax.numpy as jnp
from jax import lax
from jax.experimental import pallas as pl
from jax.experimental.pallas import tpu as pltpu
from jax.sharding import PartitionSpec as P

WLEV = 2
WLAT = 6
WLON = 12
HALF_ROWS = WLAT // 2
HALF_COLS = WLON // 2
EPSILON = 1e-05
SWAPS = ("l2", "s1", "s2", "c22", "c12", "c21", "c11", "l1")
LANES = 128
MIB = 1024 * 1024
BIAS_PARTS = 3
MASKED = -1e30
F32 = jnp.float32
BF16 = jnp.bfloat16


def iota(shape, dim):
    return lax.broadcasted_iota(jnp.int32, shape, dim)


def mm(a, b):
    return lax.dot_general(a, b, (((1,), (0,)), ((), ())), preferred_element_type=F32)


def mm_nt(a, b):
    return lax.dot_general(a, b, (((1,), (1,)), ((), ())), preferred_element_type=F32)


def three_parts(values):
    parts = []
    for _ in range(BIAS_PARTS):
        part = values.astype(BF16).astype(F32)
        parts.append(part)
        values = values - part
    return parts


def layer_norm(values, gain):
    centre = jnp.mean(values, axis=-1, keepdims=True)
    shifted = values - centre
    spread = jnp.mean(shifted * shifted, axis=-1, keepdims=True)
    return shifted * lax.rsqrt(spread + EPSILON) * gain


def stack_heads(queries, low):
    zero = jnp.zeros_like(queries)
    return jnp.concatenate([jnp.where(low, queries, zero), jnp.where(low, zero, queries)], axis=0)


def soft_context(scores, values, low):
    top = functools.reduce(jnp.maximum, [jnp.max(s, axis=-1, keepdims=True) for s in scores])
    raised = [jnp.exp(s - top) for s in scores]
    total = sum(jnp.sum(r, axis=-1, keepdims=True) for r in raised)
    context = sum(mm(r.astype(BF16), v) for r, v in zip(raised, values, strict=True)) * (1.0 / total)
    half = context.shape[0] // 2
    return jnp.where(low, context[:half], context[half:]).astype(BF16)


def attend(queries, keys, values, head_dim):
    low = iota((1, LANES), 1) < head_dim
    scaled = queries * jnp.asarray(head_dim**-0.5, BF16)
    pairs = []
    for start in range(0, queries.shape[1], LANES):
        lanes = slice(start, start + LANES)
        scores = mm_nt(stack_heads(scaled[:, lanes], low), keys[:, lanes])
        pairs.append(soft_context([scores], [values[:, lanes]], low))
    return jnp.concatenate(pairs, axis=1)


def feature_var(index, local_vars, patch):
    features = local_vars * patch
    result = jnp.where(index < features, index // patch, 0)
    for part in range(BIAS_PARTS):
        first = features + part * local_vars
        result = jnp.where((index >= first) & (index < first + local_vars), index - first, result)
    return result


def pack_kernel(
    fields_ref, *refs, band_axes, band_shape,
):
    out_refs, (block_ref, rows_ref) = refs[:-2], refs[-2:]
    var_count, levels, cols, patch, rows = fields_ref.shape
    bands = block_ref.shape[0]
    features = var_count * patch
    run = HALF_ROWS * HALF_COLS
    block = levels * run
    row_ids = iota((rows * HALF_COLS, rows), 0)
    col_ids = iota((rows * HALF_COLS, rows), 1)
    wanted = (row_ids // run) * HALF_ROWS + (row_ids % run) // HALF_COLS
    picks = [
        ((row_ids % HALF_COLS == step) & (wanted == col_ids)).astype(F32).astype(BF16)
        for step in range(HALF_COLS)
    ]
    for level in range(levels):
        for col in range(2):
            total = None
            for step in range(HALF_COLS):
                tile = fields_ref[:, level, col * HALF_COLS + step].reshape(features, rows)
                part = mm_nt(picks[step], tile)
                total = part if total is None else total + part
            for band in range(bands):
                for row in range(2):
                    source = (band * 2 + row) * run
                    target = (row * 2 + col) * block + level * run
                    block_ref[band, target : target + run, :features] = total[source : source + run]
    lane = iota((1, LANES), 1)
    row_sets = rows_ref.shape[0] // block
    for lat_step, out_ref in enumerate(out_refs):
        for var_step in range(band_shape[0]):
            band = distant_band(band_axes, band_shape, var_step, lat_step)
            pieces = [[] for _ in range(row_sets + 1)]
            for place in range(4):
                first, offset = divmod(place * features, LANES)
                data = block_ref[band, place * block : (place + 1) * block, :]
                data = pltpu.roll(data, offset, axis=1) if offset else data
                pieces[first].append((offset, data))
                if offset + features > LANES:
                    pieces[first + 1].append((0, data))
            for index in range(row_sets):
                merged = None
                for offset, data in pieces[index]:
                    merged = data if merged is None else jnp.where(lane >= offset, data, merged)
                rows_ref[index * block : (index + 1) * block, :] = merged
            out_ref[var_step] = rows_ref[...].astype(BF16)


def distant_band(band_axes, band_shape, var_step, lat_step):
    var = (lax.axis_index(band_axes[0]) + var_step) % band_shape[0]
    lat = (lax.axis_index(band_axes[1]) + lat_step) % band_shape[1]
    return var * band_shape[1] + lat


def table_kernel(
    own_hbm, table_hbm, table_bias_hbm, value_bias_hbm, value_hbm, spread_ref, value_ref,
    table_ref, table_bias_ref, value_bias_ref, sems,
    *, head_count, band_axes, band_shape, patch,
):
    all_vars, width = value_bias_hbm.shape
    bands = band_shape[0] * band_shape[1]
    smalls = ((table_hbm, table_ref), (table_bias_hbm, table_bias_ref), (value_bias_hbm, value_bias_ref))
    smalls = [pltpu.make_async_copy(a, b, sems.at[bands + i]) for i, (a, b) in enumerate(smalls)]
    for copy in smalls:
        copy.start()
    local_vars = all_vars // bands
    features = local_vars * patch
    used = features + BIAS_PARTS * local_vars
    senders = [
        distant_band(band_axes, band_shape, band_shape[0] - var_step, band_shape[1] - lat_step)
        for var_step in range(band_shape[0])
        for lat_step in range(band_shape[1])
    ]
    copies = []
    for index, sender in enumerate(senders):
        source = value_hbm.at[pl.ds(pl.multiple_of(sender * features, patch), features)]
        copies.append(pltpu.make_async_copy(source, value_ref.at[pl.ds(index * LANES, features)], sems.at[index]))
    for copy in copies:
        copy.start()

    def owners(shape, per_sender, start):
        row = iota(shape, 0)
        feature = row % per_sender + start
        owner = feature_var(feature, local_vars, patch)
        for index, sender in enumerate(senders):
            owner = jnp.where(row // per_sender == index, owner + sender * local_vars, owner)
        return owner, feature

    for copy in smalls:
        copy.wait()
    rest = LANES - features
    shape = (bands * rest, all_vars)
    owner, feature = owners(shape, rest, features)
    owned = (owner == iota(shape, 1)) & (feature < used)
    biases = None
    for index, part in enumerate(three_parts(value_bias_ref[...])):
        chosen = owned & ((feature - features) // local_vars == index)
        rows = mm(chosen.astype(F32).astype(BF16), part.astype(BF16))
        biases = rows if biases is None else biases + rows
    for index in range(bands):
        value_ref[index * LANES + features : (index + 1) * LANES, :] = biases[index * rest : (index + 1) * rest].astype(BF16)

    bias_rows = jnp.concatenate(three_parts(table_bias_ref[...]), axis=0).astype(BF16)
    stacked = jnp.concatenate([table_ref[...], bias_rows], axis=0)
    depth = stacked.shape[0]
    shape = (bands * LANES, all_vars)
    owner, feature = owners(shape, LANES, 0)
    picks = ((owner == iota(shape, 1)) & (feature < used)).astype(F32).astype(BF16)
    row = iota((bands * LANES, depth), 0) % LANES
    slot = jnp.where(row < features, row % patch, patch + (row - features) // local_vars)
    chosen = (iota((bands * LANES, depth), 1) // head_count) == slot
    table = jnp.where(chosen, mm_nt(picks, stacked), 0.0).astype(BF16)
    width_out = head_count * LANES
    select = (iota((depth, width_out), 0) % head_count == iota((depth, width_out), 1) // LANES).astype(F32).astype(BF16)
    same = feature_var(iota((LANES, LANES), 0), local_vars, patch) == feature_var(
        iota((LANES, LANES), 1), local_vars, patch
    )
    same = jnp.concatenate([same.astype(F32)] * head_count, axis=1)
    for index in range(bands):
        rows = slice(index * LANES, (index + 1) * LANES)
        spread_ref[rows, :] = (mm(table[rows], select) * same).astype(BF16)
    for copy in copies:
        copy.wait()


def relay_kernel(*refs, lat_steps):
    for index, out_ref in enumerate(refs[lat_steps + 1 :]):
        for lat_step in range(lat_steps):
            out_ref[lat_step] = refs[lat_step][index + 1]


def unpack(blocks, rows_ref, cells_ref, block, features):
    lane = iota((1, LANES), 1)
    for index, (ref, place_in_ref) in enumerate(blocks):
        rows_ref[...] = ref[place_in_ref].astype(F32)
        for place in range(4):
            first, offset = divmod(place * features, LANES)
            data = rows_ref[first * block : (first + 1) * block, :]
            if offset + features > LANES:
                data = jnp.where(lane >= offset, data, rows_ref[(first + 1) * block : (first + 2) * block, :])
            data = pltpu.roll(data, LANES - offset, axis=1) if offset else data
            cells_ref[index, place * block : (place + 1) * block, :] = jnp.where(lane < features, data, 1.0)


def pool(cells_ref, spread_ref, value_ref, score_ref, local_vars, features, head_count):
    bands = cells_ref.shape[0]
    width = value_ref.shape[1]
    tops = None
    for band in range(bands):
        scores = mm(cells_ref[band].astype(BF16), spread_ref[band * LANES : (band + 1) * LANES, :])
        score_ref[band] = scores
        tops = scores if tops is None else jnp.maximum(tops, scores)

    group = 2
    row = iota((group * LANES, LANES), 0) % LANES
    ones = ((row >= features) & (row < features + local_vars)).astype(F32).astype(BF16)
    head_dim = width // head_count
    low = iota((1, LANES), 1) < head_dim
    pooled = []
    for start in range(0, width, LANES):
        outs = []
        for side in range(2):
            head = start // head_dim + side
            columns = slice(head * LANES, (head + 1) * LANES)
            top = jnp.max(tops[:, columns], axis=-1, keepdims=True)
            total = None
            for first in range(0, bands, group):
                terms = [
                    (jnp.exp(score_ref[band, :, columns] - top) * cells_ref[band]).astype(BF16)
                    for band in range(first, first + group)
                ]
                right = jnp.concatenate(
                    [value_ref[first * LANES : (first + group) * LANES, start : start + LANES], ones], axis=1
                )
                part = mm(jnp.concatenate(terms, axis=1), right)
                total = part if total is None else total + part
            outs.append(total[:, :LANES] * (1.0 / total[:, LANES:]))
        pooled.append(jnp.where(low, outs[0], outs[1]).astype(BF16))
    return jnp.concatenate(pooled, axis=1)


def first_kernel(*refs, local_vars, features, head_count, lon_axis, band_axes, band_shape):
    var_steps, lat_steps = band_shape
    received, refs = refs[: lat_steps + var_steps - 1], refs[lat_steps + var_steps - 1 :]
    blocks = [(received[lat_step], 0) for lat_step in range(lat_steps)]
    blocks += [(ref, lat_step) for ref in received[lat_steps:] for lat_step in range(lat_steps)]
    spread_ref, value_ref, gains_hbm, agg_hbm, qkv_hbm, proj_hbm, up_hbm, down_hbm, normed_ref, latent_ref = refs[:10]
    send_refs, scratch_refs = refs[10 : 10 + len(SWAPS)], refs[10 + len(SWAPS) :]
    l1_ref, l2_ref, s1_ref, s2_ref, c11_ref, c12_ref, c21_ref, c22_ref = by_name(send_refs)
    (
        rows_ref, cells_ref, score_ref, gains_ref, agg_ref, qkv_ref, proj_ref, up_ref, down_ref, own_ref, sems,
    ) = scratch_refs
    pairs = (
        (agg_hbm, agg_ref),
        (gains_hbm, gains_ref),
        (qkv_hbm.at[0], qkv_ref),
        (proj_hbm.at[0], proj_ref),
        (up_hbm, up_ref),
        (down_hbm, down_ref),
    )
    weights = [pltpu.make_async_copy(a, b, sems.at[i]) for i, (a, b) in enumerate(pairs)]
    for copy in weights:
        copy.start()
    width = agg_hbm.shape[0]
    block = cells_ref.shape[1] // 4
    unpack(blocks, rows_ref, cells_ref, block, features)
    pooled = pool(cells_ref, spread_ref, value_ref, score_ref, local_vars, features, head_count)
    weights[0].wait()
    latent = mm(pooled, agg_ref[...])
    weights[1].wait()
    normed = layer_norm(latent, gains_ref[0:1, :]).astype(BF16)
    weights[2].wait()
    qkv = mm(normed, qkv_ref[...]).astype(BF16)
    context = attend(qkv[:, :width], qkv[:, width : 2 * width], qkv[:, 2 * width :], width // head_count)
    weights[3].wait()
    hidden = latent + mm(context, proj_ref[...])
    mixed = layer_norm(hidden, gains_ref[1:2, :]).astype(BF16)
    weights[4].wait()
    active = jax.nn.gelu(mm(mixed, up_ref[...]), approximate=True).astype(BF16)
    weights[5].wait()
    latent = hidden + mm(active, down_ref[...])
    latent_ref[...] = latent
    own = layer_norm(latent, gains_ref[2:3, :])
    normed_ref[...] = own.astype(BF16)
    own_ref[...] = own

    lon_even = lax.axis_index(lon_axis) % 2 == 0
    band_even = lax.axis_index(band_axes) % 2 == 0
    b00, b01, b10, b11 = (own_ref[i * block : (i + 1) * block, :] for i in range(4))
    side0, other0 = jnp.where(lon_even, b01, b00), jnp.where(lon_even, b00, b01)
    side1, other1 = jnp.where(lon_even, b11, b10), jnp.where(lon_even, b10, b11)
    for ref, (top, bottom) in ((l1_ref, (side0, side1)), (l2_ref, (other0, other1))):
        own_ref[:block, :] = top
        own_ref[block : 2 * block, :] = bottom
        ref[...] = own_ref[: 2 * block, :].astype(BF16)
    half = cells_ref.shape[1] // 2
    upper, lower = normed_ref[:half, :], normed_ref[half:, :]
    s1_ref[...] = jnp.where(band_even, lower, upper)
    s2_ref[...] = jnp.where(band_even, upper, lower)
    c11_ref[...] = jnp.where(band_even, side1, side0).astype(BF16)
    c12_ref[...] = jnp.where(band_even, other1, other0).astype(BF16)
    c21_ref[...] = jnp.where(band_even, side0, side1).astype(BF16)
    c22_ref[...] = jnp.where(band_even, other0, other1).astype(BF16)


def own_kernel(normed_ref, qkv_ref, query_ref, key_ref, value_ref, stack_ref, *, head_count):
    cells, width = normed_ref.shape
    half = cells // 2
    head_dim = width // head_count
    low = iota((1, LANES), 1) < head_dim
    qkv = mm(normed_ref[...], qkv_ref[1])
    queries = qkv[:, :width].astype(BF16).astype(F32) * head_dim**-0.5
    for group in range(2):
        rows = slice(group * half, (group + 1) * half)
        key_ref[group] = qkv[rows, width : 2 * width].astype(BF16)
        value_ref[group] = qkv[rows, 2 * width :].astype(BF16)
        for pair in range(width // LANES):
            stack_ref[...] = stack_heads(queries[rows, pair * LANES : (pair + 1) * LANES], low)
            query_ref[group, pair] = stack_ref[...].astype(BF16)


def second_kernel(
    query_ref, key_ref, value_ref, latent_ref, *refs, head_count, lon_axis, band_axes,
):
    l1_ref, l2_ref, s1_ref, s2_ref, c11_ref, c12_ref, c21_ref, c22_ref = by_name(refs[: len(SWAPS)])
    gains_ref, bias_ref, qkv_ref, proj_ref, decode_ref, out_ref, frame_ref, cells_ref = refs[len(SWAPS) :]
    levels = out_ref.shape[2]
    cells, width = latent_ref.shape
    half = cells // 2
    head_dim = width // head_count
    run = HALF_ROWS * HALF_COLS
    block = levels * run
    halo = 6 * block
    lon_even = lax.axis_index(lon_axis) % 2 == 0
    band = lax.axis_index(band_axes)
    band_even = band % 2 == 0
    edges = (band == 0, band == lax.axis_size(band_axes) - 1)

    for group in range(2):
        start = group * halo
        swapped = band_even if group == 0 else jnp.logical_not(band_even)
        frame_ref[start : start + block, :] = l1_ref[group * block : (group + 1) * block, :].astype(F32)
        frame_ref[start + block : start + 2 * block, :] = l2_ref[group * block : (group + 1) * block, :].astype(F32)
        line = jnp.where(swapped, s2_ref[...], s1_ref[...])
        frame_ref[start + 2 * block : start + 4 * block, :] = line.astype(F32)
        frame_ref[start + 4 * block : start + 5 * block, :] = jnp.where(swapped, c21_ref[...], c11_ref[...]).astype(F32)
        frame_ref[start + 5 * block : start + 6 * block, :] = jnp.where(swapped, c22_ref[...], c12_ref[...]).astype(F32)
    keys_vals = mm(frame_ref[...].astype(BF16), qkv_ref[1, :, width:])

    def level_of(index):
        return ((index % block) // run + WLEV // 2) // WLEV

    first = jnp.where(lon_even, 1, 0)
    query = iota((2 * half, 1), 0) % half
    own_key = iota((1, half), 1)
    own_allowed = (query // block * levels + level_of(query)) == (own_key // block * levels + level_of(own_key))
    key = iota((1, halo), 1)
    place = key // block
    side = jnp.where((place == 0) | (place == 4), first, jnp.where((place == 1) | (place == 5), 1 - first, place - 2))
    low = iota((1, LANES), 1) < head_dim
    groups = []
    for group in range(2):
        missing = (place >= 2) & edges[group]
        key_id = jnp.where(missing, -1, side * levels + level_of(key))
        allowed = (query // block * levels + level_of(query)) == key_id
        halo_keys = keys_vals[group * halo : (group + 1) * halo, :width].astype(BF16)
        halo_values = keys_vals[group * halo : (group + 1) * halo, width:].astype(BF16)
        pairs = []
        for pair in range(width // LANES):
            lanes = slice(pair * LANES, (pair + 1) * LANES)
            queries = query_ref[group, pair]
            scores = [
                jnp.where(own_allowed, mm_nt(queries, key_ref[group, :, lanes]), MASKED),
                jnp.where(allowed, mm_nt(queries, halo_keys[:, lanes]), MASKED),
            ]
            pairs.append(soft_context(scores, [value_ref[group, :, lanes], halo_values[:, lanes]], low))
        groups.append(mm(jnp.concatenate(pairs, axis=1), proj_ref[1]))
    latent = latent_ref[...] + jnp.concatenate(groups, axis=0)
    final = layer_norm(latent, gains_ref[3:4, :]).astype(BF16)
    decoded = mm(final, decode_ref[...]) + bias_ref[...].reshape(1, -1)
    for index in range(cells_ref.shape[0]):
        cells_ref[index] = decoded[:, index * LANES : (index + 1) * LANES]
    for place in range(4):
        for cell in range(run):
            source = place * block + cell
            out_row = (place // 2) * HALF_ROWS + cell // HALF_COLS
            out_col = (place % 2) * HALF_COLS + cell % HALF_COLS
            for index in range(cells_ref.shape[0]):
                piece = cells_ref[index, pl.ds(source, levels, stride=run), :].astype(BF16)
                out_ref[out_row, out_col, :, index * LANES : (index + 1) * LANES] = piece


def by_name(refs):
    return [refs[SWAPS.index(name)] for name in ("l1", "l2", "s1", "s2", "c11", "c12", "c21", "c22")]


def swap_first(index, size):
    return index ^ 1 if (index ^ 1) < size else index


def swap_second(index, size, wrap):
    other = ((index + 1) ^ 1) - 1
    if wrap:
        return other % size
    return other if 0 <= other < size else index


def per_device(
    fields, score_table, score_bias, value_table, value_bias, agg_weight, qkv_weight, proj_weight, up_weight,
    down_weight, norm_gains, decode_weight, decode_bias, *, mesh_shape,
):
    band_axes = ("var", "lat")
    lon_axis = "lon"
    sizes = [mesh_shape[name] for name in ("var", "lon", "lat")]
    bands = sizes[0] * sizes[2]
    local_vars, levels, all_rows, cols, patch = fields.shape
    all_vars, _, head_count = score_table.shape
    width = agg_weight.shape[0]
    hidden_width = up_weight.shape[1]
    out_width = decode_weight.shape[1]
    rows = all_rows // bands
    cells = levels * rows * cols
    block = levels * HALF_ROWS * HALF_COLS
    features = local_vars * patch
    assert rows == WLAT and cols == WLON and levels % WLEV == 0 and features + BIAS_PARTS * local_vars <= LANES
    packed_rows = -(-4 * features // LANES) * block
    vmem = pl.BlockSpec(memory_space=pltpu.VMEM)
    hbm = pl.BlockSpec(memory_space=pltpu.HBM)

    def in_hbm(*arrays):
        return [pltpu.with_memory_space_constraint(array, pltpu.HBM) for array in arrays]

    band_shape = (sizes[0], sizes[2])
    place = {"band_axes": band_axes, "band_shape": band_shape}
    own_blocks, *lat_blocks = pl.pallas_call(
        functools.partial(pack_kernel, **place),
        out_shape=[jax.ShapeDtypeStruct((band_shape[0], packed_rows, LANES), BF16)] * band_shape[1],
        in_specs=[vmem],
        out_specs=[vmem] * band_shape[1],
        scratch_shapes=[pltpu.VMEM((bands, cells, LANES), F32), pltpu.VMEM((packed_rows, LANES), F32)],
        compiler_params=pltpu.CompilerParams(vmem_limit_bytes=10 * MIB),
        name="pack",
    )(fields.transpose(0, 1, 3, 4, 2))

    def shift(array, axis, step):
        size = mesh_shape[axis]
        return lax.ppermute(array, axis, [(index, (index + step) % size) for index in range(size)])

    lat_blocks = [shift(array, band_axes[1], step + 1) for step, array in enumerate(lat_blocks)]
    spread, values = pl.pallas_call(
        functools.partial(table_kernel, head_count=head_count, patch=patch, **place),
        out_shape=[
            jax.ShapeDtypeStruct((bands * LANES, head_count * LANES), BF16),
            jax.ShapeDtypeStruct((bands * LANES, width), BF16),
        ],
        in_specs=[pl.BlockSpec(memory_space=pl.ANY)] + [hbm] * 4,
        out_specs=[vmem] * 2,
        scratch_shapes=[
            pltpu.VMEM((patch * head_count, all_vars), BF16),
            pltpu.VMEM((head_count, all_vars), F32),
            pltpu.VMEM((all_vars, width), F32),
            pltpu.SemaphoreType.DMA((bands + 3,)),
        ],
        compiler_params=pltpu.CompilerParams(vmem_limit_bytes=16 * MIB),
        cost_estimate=pl.CostEstimate(flops=4 * 10**9, transcendentals=0, bytes_accessed=4 * MIB),
        name="tables",
    )(
        own_blocks,
        *in_hbm(
            score_table.transpose(1, 2, 0).reshape(patch * head_count, all_vars),
            score_bias.T,
            value_bias,
            value_table.reshape(all_vars * patch, width),
        ),
    )
    relayed = pl.pallas_call(
        functools.partial(relay_kernel, lat_steps=band_shape[1]),
        out_shape=[jax.ShapeDtypeStruct((band_shape[1], packed_rows, LANES), BF16)] * (band_shape[0] - 1),
        in_specs=[vmem] * band_shape[1] + [pl.BlockSpec(memory_space=pl.ANY)],
        out_specs=[vmem] * (band_shape[0] - 1),
        compiler_params=pltpu.CompilerParams(vmem_limit_bytes=8 * MIB),
        name="relay",
    )(own_blocks, *lat_blocks, values)
    received = [own_blocks, *lat_blocks]
    received += [shift(array, band_axes[0], step + 1) for step, array in enumerate(relayed)]

    pair = (2 * block, width)
    corner = (block, width)
    structs = [jax.ShapeDtypeStruct((cells, width), BF16), jax.ShapeDtypeStruct((cells, width), F32)]
    structs += [jax.ShapeDtypeStruct(corner if name[0] == "c" else pair, BF16) for name in SWAPS]
    normed, latent, *sends = pl.pallas_call(
        functools.partial(
            first_kernel, local_vars=local_vars, features=features, head_count=head_count, lon_axis=lon_axis, **place
        ),
        out_shape=structs,
        in_specs=[vmem] * (len(received) + 2) + [hbm] * 6,
        out_specs=[vmem] * len(structs),
        scratch_shapes=[
            pltpu.VMEM((packed_rows, LANES), F32),
            pltpu.VMEM((bands, cells, LANES), F32),
            pltpu.VMEM((bands, cells, head_count * LANES), F32),
            pltpu.VMEM(norm_gains.shape, F32),
            pltpu.VMEM((width, width), BF16),
            pltpu.VMEM((width, 3 * width), BF16),
            pltpu.VMEM((width, width), BF16),
            pltpu.VMEM((width, hidden_width), BF16),
            pltpu.VMEM((hidden_width, width), BF16),
            pltpu.VMEM((cells, width), F32),
            pltpu.SemaphoreType.DMA((6,)),
        ],
        compiler_params=pltpu.CompilerParams(vmem_limit_bytes=26 * MIB),
        name="first",
    )(
        *received, spread, values,
        *in_hbm(norm_gains, agg_weight, qkv_weight, proj_weight, up_weight, down_weight),
    )

    def swap(array, band_to, lon_to):
        pairs = []
        for var in range(sizes[0]):
            for lon in range(sizes[1]):
                for lat in range(sizes[2]):
                    band = band_to(var * sizes[2] + lat)
                    other = ((band // sizes[2]) * sizes[1] + lon_to(lon)) * sizes[2] + band % sizes[2]
                    pairs.append(((var * sizes[1] + lon) * sizes[2] + lat, other))
        return lax.ppermute(array, ("var", "lon", "lat"), pairs)

    def stay(index):
        return index

    band1 = functools.partial(swap_first, size=bands)
    band2 = functools.partial(swap_second, size=bands, wrap=False)
    lon1 = functools.partial(swap_first, size=sizes[1])
    lon2 = functools.partial(swap_second, size=sizes[1], wrap=True)
    moves = {"l1": (stay, lon1), "l2": (stay, lon2), "s1": (band1, stay), "s2": (band2, stay)}
    moves |= {"c11": (band1, lon1), "c12": (band1, lon2), "c21": (band2, lon1), "c22": (band2, lon2)}
    halos = [swap(array, *moves[name]) for array, name in zip(sends, SWAPS, strict=True)]

    half = cells // 2
    queries, keys, vals = pl.pallas_call(
        functools.partial(own_kernel, head_count=head_count),
        out_shape=[
            jax.ShapeDtypeStruct((2, width // LANES, cells, LANES), BF16),
            jax.ShapeDtypeStruct((2, half, width), BF16),
            jax.ShapeDtypeStruct((2, half, width), BF16),
        ],
        in_specs=[vmem] * 2,
        out_specs=[vmem] * 3,
        scratch_shapes=[pltpu.VMEM((cells, LANES), F32)],
        compiler_params=pltpu.CompilerParams(vmem_limit_bytes=12 * MIB),
        name="own",
    )(normed, qkv_weight)
    forecast = pl.pallas_call(
        functools.partial(second_kernel, head_count=head_count, lon_axis=lon_axis, band_axes=band_axes),
        out_shape=jax.ShapeDtypeStruct((rows, cols, levels, out_width), BF16),
        in_specs=[vmem] * 17,
        out_specs=vmem,
        scratch_shapes=[pltpu.VMEM((12 * block, width), F32), pltpu.VMEM((out_width // LANES, cells, LANES), F32)],
        compiler_params=pltpu.CompilerParams(vmem_limit_bytes=20 * MIB),
        name="second",
    )(queries, keys, vals, latent, *halos, norm_gains, decode_bias, qkv_weight, proj_weight, decode_weight)
    return forecast.transpose(2, 0, 1, 3)


def solution(mesh):
    shape = dict(mesh.shape)
    return jax.shard_map(
        functools.partial(per_device, mesh_shape=shape),
        mesh=mesh,
        in_specs=(P(("var", "lat"), None, None, "lon", None),) + (P(),) * 12,
        out_specs=P(None, ("var", "lat"), "lon", None),
        check_vma=False,
    )
```
